32 devices in a mesh: slab: 2 (over x), row: 8 (over z, y), col: 2 (over core).
Axes of the slice: x: 2, y: 2, z: 4, core: 2. Of those that a mesh axis runs over, the one named last changes fastest.
Arguments:
- image: float32 [1024, 4096], P(('slab', 'row'), 'col'), parts along dimension 0, may hold values from -6 to 6
Outputs:
- dog_fine: bfloat16 [4, 1024, 4096], P(None, ('slab', 'row'), 'col'), parts along dimension 1
- hessian_fine: bfloat16 [2, 1024, 4096], P(None, ('slab', 'row'), 'col'), parts along dimension 1
- dog_coarse: bfloat16 [4, 512, 2048], P(None, ('slab', 'row', 'col')), parts along dimension 1
- hessian_coarse: bfloat16 [2, 512, 2048], P(None, ('slab', 'row', 'col')), parts along dimension 1
The draws below stay inside these ranges and needn't reach their ends.
There are 2 independent parts, one for each index of `slab`. The reference program is written for one: setup_inputs(seed, part) draws one part's arguments, and reference() takes and returns one part's arrays. A program takes and returns all parts, laid end to end along the dimension named above; each array names one. Nothing has to cross between parts.
All inputs are finite; a program needn't handle non-finite values.
Results may differ from the reference program's by a relative error of at most 0.0013.
Values may be sent and summed in bfloat16 or wider, within the bound.
A program may use at most 64 MiB of HBM per device.

```python
import jax
import jax.numpy as jnp
from jax import lax

H = 512
W = 4096


def block_scale(rng, extent, split, low, largest):
    def one(dim, blocks):
        heights = jax.random.uniform(jax.random.fold_in(jax.random.fold_in(rng, 6), dim), (blocks,), jnp.float32, low / len(split), largest / len(split))
        return jnp.repeat(jnp.exp(heights), extent[dim] // blocks).reshape((-1,) + (1,) * (len(extent) - dim - 1))

    loudness = one(*split[0])
    for cut in split[1:]:
        loudness = loudness * one(*cut)
    return loudness


def normal_values(own_key, extent, scale, limit, cuts=(), kind=jnp.bfloat16):
    entries = jax.random.normal(own_key, extent, jnp.float32) * scale
    if len(cuts) > 0:
        entries = block_scale(own_key, extent, cuts, -0.22, 0.18) * entries
    return jnp.clip(entries, min=-limit, max=limit).astype(kind)


def setup_inputs(seed: int = 0, part: int = 0) -> dict:
    streams_of = jax.random.split(jax.random.key(seed), 2)
    part_splits = jax.random.split(jax.random.fold_in(streams_of[1], part), 2)
    return {
        "image": normal_values(part_splits[0], (H, W), 1.0, 6.0, ((0, 8), (1, 2)), jnp.float32),
    }


SIGMAS = [1.6 * 2.0 ** (k / 4.0) for k in range(5)]


def taps(sigma):
    offset = jnp.arange(25).astype(jnp.float32) - 12.0
    weights = jnp.exp(-offset * offset / (2.0 * sigma * sigma))
    return weights / jnp.sum(weights)


def blur(field, sigma):
    kernel = taps(sigma)
    data = field[None, None]
    vertical = lax.conv_general_dilated(data, kernel[None, None, :, None], (1, 1), ((12, 12), (0, 0)), precision=lax.Precision.HIGHEST)
    both = lax.conv_general_dilated(vertical, kernel[None, None, None, :], (1, 1), ((0, 0), (12, 12)), precision=lax.Precision.HIGHEST)
    return both[0, 0]


def hessian(diff):
    padded = jnp.pad(diff, 1)
    dxx = padded[1:-1, 2:] + padded[1:-1, :-2] - 2.0 * diff
    dyy = padded[2:, 1:-1] + padded[:-2, 1:-1] - 2.0 * diff
    dxy = (padded[2:, 2:] - padded[2:, :-2] - padded[:-2, 2:] + padded[:-2, :-2]) / 4.0
    return dxx * dyy - dxy * dxy


def octave(base, dog_gain, hess_gain):
    levels = [blur(base, s) for s in SIGMAS]
    diffs = [levels[k + 1] - levels[k] for k in range(4)]
    dogs = jnp.stack([(dog_gain * d).astype(jnp.bfloat16) for d in diffs])
    hess = jnp.stack([(hess_gain * hessian(diffs[m + 1])).astype(jnp.bfloat16) for m in range(2)])
    return dogs, hess, levels[4]


def reference(image):
    dog_fine, hessian_fine, top_level = octave(image, 20.0, 5000.0)
    coarse_base = top_level[0::2, 0::2]
    dog_coarse, hessian_coarse, unused = octave(coarse_base, 80.0, 200000.0)
    return dog_fine, hessian_fine, dog_coarse, hessian_coarse
```

```python
import functools

import jax
import jax.numpy as jnp
import numpy as np
from jax import lax
from jax.experimental import pallas as pl
from jax.experimental.pallas import tpu as pltpu
from jax.sharding import PartitionSpec as P

SIGMAS = [1.6 * 2.0 ** (k / 4.0) for k in range(5)]
LEVELS = 5
LANE = 128
HALF = LANE // 2
RIM = 16
MESH = pl.DeviceIdType.MESH
BF = jnp.bfloat16
F32 = jnp.float32


def taps_at(sigma, offset):
    spread = np.arange(25, dtype=np.float64) - 12.0
    total = np.sum(np.exp(-spread * spread / (2.0 * sigma * sigma)))
    weight = np.exp(-(offset**2) / (2.0 * sigma * sigma)) / total
    return np.where(np.abs(offset) <= 12, weight, 0.0)


def halves(matrix):
    high = matrix.astype(BF)
    low = (matrix - high.astype(np.float64)).astype(BF)
    return high, low


def ring_rows(count):
    rows = np.full(count + 8, 10**6, dtype=np.float64)
    rows[: count + 1] = np.arange(count + 1)
    rows[-1] = -1
    return rows


def ring_inputs(count, before):
    total = np.arange(count, dtype=np.float64)
    return np.where(total >= count - before, total - count, total)


def vertical_matrix(out_rows, in_rows, sigma):
    return taps_at(sigma, in_rows[None, :] - out_rows[:, None])


def pad_rows(matrix, multiple):
    return np.pad(matrix, ((0, -matrix.shape[0] % multiple), (0, 0)))


def column_weights(matrix):
    high, low = halves(matrix)
    pair = np.concatenate([high, low], axis=1)
    return np.concatenate([pair, pair], axis=0)


def row_weights(matrix):
    high, low = halves(pad_rows(matrix, 16))
    return np.concatenate([high, high, low, low], axis=1)


def split(x):
    high = x.astype(BF)
    low = (x - high.astype(F32)).astype(BF)
    return high, low


def kernel(
    rows_total, image, a_fine, a_coarse, g_level, g_base,
    dog_fine, hess_fine, dog_coarse, hess_coarse,
    ext, cext, vert, lev, diff, base,
    load_sem, fsend, frecv, csend, crecv,
):
    tile_rows, tile_cols = image.shape
    tiles = tile_cols // LANE
    strip = tile_rows // 4
    half_cols = tile_cols // 2
    r = lax.axis_index("row")
    c = lax.axis_index("col")
    other = 1 - c
    has_up = r > 0
    has_down = r < rows_total - 1

    load = pltpu.make_async_copy(image, ext.at[pl.ds(0, tile_rows), pl.ds(0, tile_cols)], load_sem)
    load.start()

    barrier = pltpu.get_barrier_semaphore()

    def greet(row, col):
        pl.semaphore_signal(barrier, inc=1, device_id={"row": row, "col": col}, device_id_type=MESH)

    greet(r, other)

    @pl.when(has_up)
    def _():
        greet(r - 1, c)
        greet(r - 1, other)

    @pl.when(has_down)
    def _():
        greet(r + 1, c)
        greet(r + 1, other)

    ends = (r == 0).astype(jnp.int32) + (r == rows_total - 1).astype(jnp.int32)
    pl.semaphore_wait(barrier, 5 - 2 * ends)

    load.wait()

    def remote(src, dst, send, recv, row, col):
        return pltpu.make_async_remote_copy(
            src_ref=src, dst_ref=dst, send_sem=send, recv_sem=recv,
            device_id={"row": row, "col": col}, device_id_type=MESH,
        )

    edge = pl.ds(pl.multiple_of(other * (tile_cols - LANE), LANE), LANE)
    own = pl.ds(0, tile_cols)
    rim = pl.ds(tile_cols, LANE)
    first = pl.ds(0, RIM)
    last = pl.ds(tile_rows - RIM, RIM)
    below = pl.ds(tile_rows, RIM)
    above = pl.ds(tile_rows + RIM, RIM)
    inner = pl.ds(0, tile_rows)

    to_down = remote(ext.at[last, own], ext.at[above, own], fsend.at[0], frecv.at[0], r + 1, c)
    to_down_corner = remote(ext.at[last, edge], ext.at[above, rim], fsend.at[1], frecv.at[1], r + 1, other)
    to_up = remote(ext.at[first, own], ext.at[below, own], fsend.at[2], frecv.at[2], r - 1, c)
    to_up_corner = remote(ext.at[first, edge], ext.at[below, rim], fsend.at[3], frecv.at[3], r - 1, other)
    to_side = remote(ext.at[inner, edge], ext.at[inner, rim], fsend.at[4], frecv.at[4], r, other)

    @pl.when(has_down)
    def _():
        to_down.start()
        to_down_corner.start()

    @pl.when(has_up)
    def _():
        to_up.start()
        to_up_corner.start()

    to_side.start()

    wide = tile_cols + LANE

    @pl.when(r == 0)
    def _():
        ext[above, :] = jnp.zeros((RIM, wide), F32)

    @pl.when(r == rows_total - 1)
    def _():
        ext[below, :] = jnp.zeros((RIM, wide), F32)

    cext[:, pl.ds(tile_cols, LANE)] = jnp.zeros((3 * strip, LANE), F32)

    @pl.when(jnp.logical_and(r == 0, c == 0))
    def _():
        cext[pl.ds(2 * strip, strip), own] = jnp.zeros((strip, tile_cols), F32)

    @pl.when(jnp.logical_and(r == rows_total - 1, c == 1))
    def _():
        cext[pl.ds(strip, strip), own] = jnp.zeros((strip, tile_cols), F32)

    to_side.wait()

    @pl.when(has_up)
    def _():
        to_down.wait_recv()
        to_down_corner.wait_recv()

    @pl.when(has_down)
    def _():
        to_up.wait_recv()
        to_up_corner.wait_recv()

    lane = lax.broadcasted_iota(jnp.int32, (1, LANE), 1)

    def vertical_pass(source, matrix, edge_keep):
        def tile_of(t):
            value = source[:, t * LANE : (t + 1) * LANE]
            if t == tiles:
                value = value * edge_keep
            return pltpu.roll(value, HALF, 1)

        rolled = [tile_of(t) for t in range(tiles + 1)]
        left = lane < HALF
        for t0 in range(0, tiles + 1, 4):
            group = [
                jnp.where(left, rolled[t - 1], rolled[t])
                for t in range(t0, min(t0 + 4, tiles + 1))
            ]
            high, low = split(jnp.concatenate(group, axis=1))
            stacked = jnp.concatenate([high, low, high, low], axis=0)
            count = matrix.shape[0]
            vert[pl.ds(0, count), t0 * LANE : t0 * LANE + stacked.shape[1]] = jnp.dot(
                matrix[...], stacked, preferred_element_type=F32
            )

    keep = jnp.where((lane < HALF) == (c == 0), 1.0, 0.0).astype(F32)
    vertical_pass(ext, a_fine, keep)

    half_rows = tile_rows // 2
    windows = []
    for b in range(half_cols // LANE):
        windows.append(vert[0:half_rows, 2 * b * LANE : (2 * b + 3) * LANE])
    high, low = split(jnp.concatenate(windows, axis=0))
    product = jnp.dot(jnp.concatenate([high, low], axis=1), g_base[...], preferred_element_type=F32)
    product = product[:, :LANE] + product[:, LANE:]
    for b in range(half_cols // LANE):
        base[:, b * LANE : (b + 1) * LANE] = product[b * half_rows : (b + 1) * half_rows]

    mine = pl.ds(pl.multiple_of(c * half_cols, LANE), half_cols)
    top, bottom = base.at[pl.ds(0, strip)], base.at[pl.ds(strip, strip)]

    def slot(index):
        return cext.at[pl.ds(pl.multiple_of(index * strip, 8), strip), mine]

    sends = [
        remote(top, slot(2 * other), csend.at[0], crecv.at[0], r, other),
        remote(bottom, slot(c), csend.at[1], crecv.at[1], r, other),
    ]
    up = remote(top, slot(1), csend.at[2], crecv.at[2 + c], r - 1, 1)
    down = remote(bottom, slot(2), csend.at[3], crecv.at[2 + c], r + 1, 0)

    @pl.when(has_up)
    def _():
        up.start()

    @pl.when(has_down)
    def _():
        down.start()

    for send in sends:
        send.start()

    cext[pl.ds(pl.multiple_of(2 * c * strip, 8), strip), mine] = base[0:strip]
    cext[pl.ds(pl.multiple_of(other * strip, 8), strip), mine] = base[strip : 2 * strip]

    def horizontal_pass(start, high_rows, blocks):
        for k in range(LEVELS):
            rows = pl.ds(start + k * high_rows, high_rows)
            windows = []
            for b in range(blocks):
                if b == tiles:
                    windows.append(
                        jnp.concatenate([vert[rows, b * LANE : (b + 1) * LANE], vert[rows, 0:LANE]], axis=1)
                    )
                else:
                    windows.append(vert[rows, b * LANE : (b + 2) * LANE])
            high, low = split(jnp.concatenate(windows, axis=0))
            product = jnp.dot(
                jnp.concatenate([high, low], axis=1), g_level[k], preferred_element_type=F32
            )
            lev[k, pl.ds(0, blocks * high_rows), :] = product[:, :LANE] + product[:, LANE:]

    def responses(count, blocks, dog_gain, hess_gain, row_keep, edge_keep, dog, hess):
        high_rows = count + 8
        for b in range(blocks):
            rows = pl.ds(b * high_rows, high_rows)
            level = [lev[k, rows, :] for k in range(LEVELS)]
            for k in range(LEVELS - 1):
                d = level[k + 1] - level[k]
                if b < tiles:
                    dog[k, :, b * LANE : (b + 1) * LANE] = (dog_gain * d[:count]).astype(BF)
                if k in (1, 2):
                    d = d * row_keep
                    if b == tiles:
                        d = d * edge_keep
                    diff[k - 1, rows, :] = d
        if blocks == tiles:
            diff[:, pl.ds(tiles * high_rows, high_rows), :] = jnp.zeros((2, high_rows, LANE), F32)

        def block(b):
            before, after = (b - 1) % (tiles + 1), (b + 1) % (tiles + 1)
            for m in range(2):
                centre = diff[m, pl.ds(b * high_rows, high_rows), :]
                previous = diff[m, pl.ds(before * high_rows, high_rows), :]
                following = diff[m, pl.ds(after * high_rows, high_rows), :]
                right = pltpu.roll(jnp.where(lane == 0, following, centre), LANE - 1, 1)
                left = pltpu.roll(jnp.where(lane == LANE - 1, previous, centre), 1, 1)
                slope = right - left
                dxx = (right + left - 2.0 * centre)[:count]
                twice = 2.0 * centre
                dyy = (
                    pltpu.roll(centre, high_rows - 1, 0) + pltpu.roll(centre, 1, 0) - twice
                )[:count]
                dxy = (pltpu.roll(slope, high_rows - 1, 0) - pltpu.roll(slope, 1, 0))[:count] * 0.25
                hess[m, :, b * LANE : (b + 1) * LANE] = (hess_gain * (dxx * dyy - dxy * dxy)).astype(BF)

        for b in range(tiles):
            block(b)

    def row_mask(count, before, after):
        index = lax.broadcasted_iota(jnp.int32, (count + 8, 1), 0)
        gone = jnp.logical_or(
            jnp.logical_and(index == count, jnp.logical_not(after)),
            jnp.logical_and(index == count + 7, jnp.logical_not(before)),
        )
        return jnp.where(gone, 0.0, 1.0).astype(F32)

    horizontal_pass(half_rows, tile_rows + 8, tiles + 1)
    edge_keep = jnp.where(lane == jnp.where(c == 0, 0, LANE - 1), 1.0, 0.0).astype(F32)
    responses(
        tile_rows, tiles + 1, 20.0, 5000.0,
        row_mask(tile_rows, has_up, has_down), edge_keep, dog_fine, hess_fine,
    )

    for send in sends:
        send.wait_recv()

    @pl.when(jnp.logical_or(c == 1, has_up))
    def _():
        @pl.when(jnp.logical_or(c == 0, has_down))
        def _():
            for index in range(2):
                remote(top, slot(1), csend.at[2], crecv.at[2 + index], r, other).wait_recv()

    vertical_pass(cext, a_coarse, jnp.ones((1, LANE), F32))
    horizontal_pass(0, strip + 8, tiles)
    responses(
        strip, tiles, 80.0, 200000.0,
        row_mask(strip, jnp.logical_or(has_up, c == 1), jnp.logical_or(has_down, c == 0)),
        None, dog_coarse, hess_coarse,
    )

    @pl.when(has_down)
    def _():
        to_down.wait_send()
        to_down_corner.wait_send()
        down.wait_send()

    @pl.when(has_up)
    def _():
        to_up.wait_send()
        to_up_corner.wait_send()
        up.wait_send()

    for send in sends:
        send.wait_send()


def solution(mesh):
    rows_total = mesh.shape["row"]

    def local(image):
        tile_rows, tile_cols = image.shape
        strip = tile_rows // 4
        tiles = tile_cols // LANE
        fine_in = ring_inputs(tile_rows + 2 * RIM, RIM)
        coarse_in = ring_inputs(3 * strip, strip)
        a_fine = row_weights(
            np.concatenate(
                [vertical_matrix(2.0 * np.arange(tile_rows // 2), fine_in, SIGMAS[4])]
                + [vertical_matrix(ring_rows(tile_rows), fine_in, s) for s in SIGMAS]
            )
        )
        a_coarse = row_weights(
            np.concatenate([vertical_matrix(ring_rows(strip), coarse_in, s) for s in SIGMAS])
        )
        window = np.arange(2 * LANE, dtype=np.float64)[:, None] - HALF
        g_level = np.stack(
            [column_weights(taps_at(s, window - np.arange(LANE)[None, :])) for s in SIGMAS]
        )
        wider = np.arange(3 * LANE, dtype=np.float64)[:, None] - HALF
        g_base = column_weights(taps_at(SIGMAS[4], wider - 2.0 * np.arange(LANE)[None, :]))

        vmem = pl.BlockSpec(memory_space=pltpu.VMEM)
        ring = tile_rows + 8
        wide = tile_cols + LANE
        return pl.pallas_call(
            functools.partial(kernel, rows_total),
            out_shape=(
                jax.ShapeDtypeStruct((4, tile_rows, tile_cols), BF),
                jax.ShapeDtypeStruct((2, tile_rows, tile_cols), BF),
                jax.ShapeDtypeStruct((4, strip, tile_cols), BF),
                jax.ShapeDtypeStruct((2, strip, tile_cols), BF),
            ),
            in_specs=[pl.BlockSpec(memory_space=pl.ANY)] + [vmem] * 4,
            out_specs=(vmem,) * 4,
            scratch_shapes=[
                pltpu.VMEM((tile_rows + 2 * RIM, wide), F32),
                pltpu.VMEM((3 * strip, wide), F32),
                pltpu.VMEM((a_fine.shape[0], wide), F32),
                pltpu.VMEM((LEVELS, (tiles + 1) * ring, LANE), F32),
                pltpu.VMEM((2, (tiles + 1) * ring, LANE), F32),
                pltpu.VMEM((tile_rows // 2, tile_cols // 2), F32),
                pltpu.SemaphoreType.DMA,
                pltpu.SemaphoreType.DMA((5,)),
                pltpu.SemaphoreType.DMA((5,)),
                pltpu.SemaphoreType.DMA((4,)),
                pltpu.SemaphoreType.DMA((4,)),
            ],
            compiler_params=pltpu.CompilerParams(
                collective_id=0, has_side_effects=True, vmem_limit_bytes=48 * 2**20
            ),
        )(image, a_fine, a_coarse, g_level, g_base)

    return jax.shard_map(
        local,
        mesh=mesh,
        in_specs=(P(("slab", "row"), "col"),),
        out_specs=(
            P(None, ("slab", "row"), "col"),
            P(None, ("slab", "row"), "col"),
            P(None, ("slab", "row", "col"), None),
            P(None, ("slab", "row", "col"), None),
        ),
        check_vma=False,
    )
```

```python
import functools

import jax
import jax.numpy as jnp
import numpy as np
from jax import lax
from jax.experimental import pallas as pl
from jax.experimental.pallas import tpu as pltpu
from jax.sharding import PartitionSpec as P

SIGMAS = [1.6 * 2.0 ** (k / 4.0) for k in range(5)]
LEVELS = 5
LANE = 128
HALF = LANE // 2
RIM = 16
CHUNK = 4
MESH = pl.DeviceIdType.MESH
BF = jnp.bfloat16
F32 = jnp.float32


def taps_at(sigma, offset):
    spread = np.arange(25, dtype=np.float64) - 12.0
    total = np.sum(np.exp(-spread * spread / (2.0 * sigma * sigma)))
    weight = np.exp(-(offset**2) / (2.0 * sigma * sigma)) / total
    return np.where(np.abs(offset) <= 12, weight, 0.0)


def halves(matrix):
    high = matrix.astype(BF)
    low = (matrix - high.astype(np.float64)).astype(BF)
    return high, low


def ring_rows(count):
    rows = np.full(count + 8, 10**6, dtype=np.float64)
    rows[: count + 1] = np.arange(count + 1)
    rows[-1] = -1
    return rows


def ring_inputs(count, before):
    total = np.arange(count, dtype=np.float64)
    return np.where(total >= count - before, total - count, total)


def vertical_matrix(out_rows, in_rows, sigma):
    return taps_at(sigma, in_rows[None, :] - out_rows[:, None])


def pad_rows(matrix, multiple):
    return np.pad(matrix, ((0, -matrix.shape[0] % multiple), (0, 0)))


def column_weights(matrix):
    high, low = halves(matrix)
    pair = np.concatenate([high, low], axis=1)
    return np.concatenate([pair, pair], axis=0)


def row_weights(matrix):
    high, low = halves(pad_rows(matrix, 16))
    return np.concatenate([high, high, low, low], axis=1)


def split(x):
    high = x.astype(BF)
    low = (x - high.astype(F32)).astype(BF)
    return high, low


def kernel(
    rows_total, image, a_fine_far, a_coarse_far, g_level_far, g_base_far,
    dog_fine, hess_fine, dog_coarse, hess_coarse,
    ext, cext, vert, lev, diff, base, a_fine, a_coarse, g_level, g_base,
    load_sem, fsend, frecv, csend, crecv,
):
    tile_rows, tile_cols = image.shape
    tiles = tile_cols // LANE
    strip = tile_rows // 4
    half_cols = tile_cols // 2
    r = lax.axis_index("row")
    c = lax.axis_index("col")
    other = 1 - c
    has_up = r > 0
    has_down = r < rows_total - 1

    load = pltpu.make_async_copy(image, ext.at[pl.ds(0, tile_rows), pl.ds(0, tile_cols)], load_sem.at[0])
    load.start()
    pairs = [(a_fine_far, a_fine), (g_base_far, g_base), (g_level_far, g_level), (a_coarse_far, a_coarse)]
    weights = [
        pltpu.make_async_copy(far, near, load_sem.at[1 + i]) for i, (far, near) in enumerate(pairs)
    ]

    barrier = pltpu.get_barrier_semaphore()

    def greet(row, col):
        pl.semaphore_signal(barrier, inc=1, device_id={"row": row, "col": col}, device_id_type=MESH)

    greet(r, other)

    @pl.when(has_up)
    def _():
        greet(r - 1, c)
        greet(r - 1, other)

    @pl.when(has_down)
    def _():
        greet(r + 1, c)
        greet(r + 1, other)

    ends = (r == 0).astype(jnp.int32) + (r == rows_total - 1).astype(jnp.int32)
    pl.semaphore_wait(barrier, 5 - 2 * ends)

    for weight in weights:
        weight.start()
    load.wait()

    def remote(src, dst, send, recv, row, col):
        return pltpu.make_async_remote_copy(
            src_ref=src, dst_ref=dst, send_sem=send, recv_sem=recv,
            device_id={"row": row, "col": col}, device_id_type=MESH,
        )

    edge = pl.ds(pl.multiple_of(other * (tile_cols - LANE), LANE), LANE)
    own = pl.ds(0, tile_cols)
    rim = pl.ds(tile_cols, LANE)
    first = pl.ds(0, RIM)
    last = pl.ds(tile_rows - RIM, RIM)
    below = pl.ds(tile_rows, RIM)
    above = pl.ds(tile_rows + RIM, RIM)
    inner = pl.ds(0, tile_rows)

    chunks = tiles // CHUNK
    span = CHUNK * LANE
    to_down, to_up = [], []
    for j in range(chunks):
        part = pl.ds(j * span, span)
        to_down.append(remote(ext.at[last, part], ext.at[above, part], fsend.at[2 * j], frecv.at[2 * j], r + 1, c))
        to_up.append(
            remote(ext.at[first, part], ext.at[below, part], fsend.at[2 * j + 1], frecv.at[2 * j + 1], r - 1, c)
        )
    n = 2 * chunks
    to_down_corner = remote(ext.at[last, edge], ext.at[above, rim], fsend.at[n], frecv.at[n], r + 1, other)
    to_up_corner = remote(ext.at[first, edge], ext.at[below, rim], fsend.at[n + 1], frecv.at[n + 1], r - 1, other)
    to_side = remote(ext.at[inner, edge], ext.at[inner, rim], fsend.at[n + 2], frecv.at[n + 2], r, other)

    @pl.when(has_down)
    def _():
        to_down_corner.start()
        to_down[0].start()

    @pl.when(has_up)
    def _():
        to_up_corner.start()
        for send in to_up:
            send.start()

    @pl.when(has_down)
    def _():
        for send in to_down[1:]:
            send.start()

    to_side.start()

    wide = tile_cols + LANE

    @pl.when(r == 0)
    def _():
        ext[above, :] = jnp.zeros((RIM, wide), F32)

    @pl.when(r == rows_total - 1)
    def _():
        ext[below, :] = jnp.zeros((RIM, wide), F32)

    cext[:, pl.ds(tile_cols, LANE)] = jnp.zeros((3 * strip, LANE), F32)

    @pl.when(jnp.logical_and(r == 0, c == 0))
    def _():
        cext[pl.ds(2 * strip, strip), own] = jnp.zeros((strip, tile_cols), F32)

    @pl.when(jnp.logical_and(r == rows_total - 1, c == 1))
    def _():
        cext[pl.ds(strip, strip), own] = jnp.zeros((strip, tile_cols), F32)

    for weight in weights:
        weight.wait()
    to_side.wait()

    @pl.when(has_up)
    def _():
        to_down_corner.wait_recv()

    @pl.when(has_down)
    def _():
        to_up_corner.wait_recv()

    lane = lax.broadcasted_iota(jnp.int32, (1, LANE), 1)

    def vertical_pass(source, matrix, edge_keep, begin, end):
        def tile_of(t):
            value = source[:, t * LANE : (t + 1) * LANE]
            if t == tiles:
                value = value * edge_keep
            return pltpu.roll(value, HALF, 1)

        rolled = {t: tile_of(t % (tiles + 1)) for t in range(begin - 1, end)}
        left = lane < HALF
        group = [jnp.where(left, rolled[t - 1], rolled[t]) for t in range(begin, end)]
        high, low = split(jnp.concatenate(group, axis=1))
        stacked = jnp.concatenate([high, low, high, low], axis=0)
        vert[pl.ds(0, matrix.shape[0]), begin * LANE : end * LANE] = jnp.dot(
            matrix[...], stacked, preferred_element_type=F32
        )

    def horizontal_pass(start, high_rows, begin, end):
        for k in range(LEVELS):
            rows = pl.ds(start + k * high_rows, high_rows)
            windows = []
            for b in range(begin, end):
                if b == tiles:
                    windows.append(
                        jnp.concatenate([vert[rows, b * LANE : (b + 1) * LANE], vert[rows, 0:LANE]], axis=1)
                    )
                else:
                    windows.append(vert[rows, b * LANE : (b + 2) * LANE])
            high, low = split(jnp.concatenate(windows, axis=0))
            product = jnp.dot(
                jnp.concatenate([high, low], axis=1), g_level[k], preferred_element_type=F32
            )
            lev[k, pl.ds(begin * high_rows, (end - begin) * high_rows), :] = (
                product[:, :LANE] + product[:, LANE:]
            )

    half_rows = tile_rows // 2

    def base_pass(begin, end):
        windows = [vert[0:half_rows, 2 * b * LANE : (2 * b + 3) * LANE] for b in range(begin, end)]
        high, low = split(jnp.concatenate(windows, axis=0))
        product = jnp.dot(
            jnp.concatenate([high, low], axis=1), g_base[...], preferred_element_type=F32
        )
        product = product[:, :LANE] + product[:, LANE:]
        for b in range(begin, end):
            base[:, b * LANE : (b + 1) * LANE] = product[
                (b - begin) * half_rows : (b - begin + 1) * half_rows
            ]

    keep = jnp.where((lane < HALF) == (c == 0), 1.0, 0.0).astype(F32)
    sends, ups, downs = [], [], []
    base_done = 0
    blocks_done = 0
    for j in range(chunks):

        @pl.when(has_up)
        def _():
            to_down[j].wait_recv()

        @pl.when(has_down)
        def _():
            to_up[j].wait_recv()

        ready = CHUNK * (j + 1) + (1 if j == chunks - 1 else 0)
        vertical_pass(ext, a_fine, keep, CHUNK * j, ready)
        base_end = (ready - 1) // 2
        base_pass(base_done, base_end)

        near = pl.ds(base_done * LANE, (base_end - base_done) * LANE)
        mine = pl.ds(
            pl.multiple_of(c * half_cols + base_done * LANE, LANE), (base_end - base_done) * LANE
        )
        top, bottom = base.at[pl.ds(0, strip), near], base.at[pl.ds(strip, strip), near]

        def slot_rows(index):
            return pl.ds(pl.multiple_of(index * strip, 8), strip)

        pair = [
            remote(top, cext.at[slot_rows(2 * other), mine], csend.at[4 * j], crecv.at[4 * j], r, other),
            remote(bottom, cext.at[slot_rows(c), mine], csend.at[4 * j + 1], crecv.at[4 * j + 1], r, other),
        ]
        up = remote(top, cext.at[slot_rows(1), mine], csend.at[4 * j + 2], crecv.at[4 * j + 2 + c], r - 1, 1)
        down = remote(bottom, cext.at[slot_rows(2), mine], csend.at[4 * j + 3], crecv.at[4 * j + 2 + c], r + 1, 0)
        sends += pair
        ups.append(up)
        downs.append(down)

        @pl.when(has_up)
        def _():
            up.start()

        @pl.when(has_down)
        def _():
            down.start()

        for send in pair:
            send.start()

        cext[slot_rows(2 * c), mine] = base[0:strip, near]
        cext[slot_rows(other), mine] = base[strip : 2 * strip, near]

        blocks_end = tiles + 1 if j == chunks - 1 else ready - 1
        horizontal_pass(half_rows, tile_rows + 8, blocks_done, blocks_end)
        base_done, blocks_done = base_end, blocks_end

    def responses(count, blocks, dog_gain, hess_gain, row_keep, edge_keep, dog, hess):
        high_rows = count + 8
        for b in range(blocks):
            rows = pl.ds(b * high_rows, high_rows)
            level = [lev[k, rows, :] for k in range(LEVELS)]
            for k in range(LEVELS - 1):
                d = level[k + 1] - level[k]
                if b < tiles:
                    dog[k, :, b * LANE : (b + 1) * LANE] = (dog_gain * d[:count]).astype(BF)
                if k in (1, 2):
                    d = d * row_keep
                    if b == tiles:
                        d = d * edge_keep
                    diff[k - 1, rows, :] = d
        if blocks == tiles:
            diff[:, pl.ds(tiles * high_rows, high_rows), :] = jnp.zeros((2, high_rows, LANE), F32)

        def block(b):
            before, after = (b - 1) % (tiles + 1), (b + 1) % (tiles + 1)
            for m in range(2):
                centre = diff[m, pl.ds(b * high_rows, high_rows), :]
                previous = diff[m, pl.ds(before * high_rows, high_rows), :]
                following = diff[m, pl.ds(after * high_rows, high_rows), :]
                right = pltpu.roll(jnp.where(lane == 0, following, centre), LANE - 1, 1)
                left = pltpu.roll(jnp.where(lane == LANE - 1, previous, centre), 1, 1)
                slope = right - left
                dxx = (right + left - 2.0 * centre)[:count]
                twice = 2.0 * centre
                dyy = (
                    pltpu.roll(centre, high_rows - 1, 0) + pltpu.roll(centre, 1, 0) - twice
                )[:count]
                dxy = (pltpu.roll(slope, high_rows - 1, 0) - pltpu.roll(slope, 1, 0))[:count] * 0.25
                hess[m, :, b * LANE : (b + 1) * LANE] = (hess_gain * (dxx * dyy - dxy * dxy)).astype(BF)

        for b in range(tiles):
            block(b)

    def row_mask(count, before, after):
        index = lax.broadcasted_iota(jnp.int32, (count + 8, 1), 0)
        gone = jnp.logical_or(
            jnp.logical_and(index == count, jnp.logical_not(after)),
            jnp.logical_and(index == count + 7, jnp.logical_not(before)),
        )
        return jnp.where(gone, 0.0, 1.0).astype(F32)

    edge_keep = jnp.where(lane == jnp.where(c == 0, 0, LANE - 1), 1.0, 0.0).astype(F32)
    responses(
        tile_rows, tiles + 1, 20.0, 5000.0,
        row_mask(tile_rows, has_up, has_down), edge_keep, dog_fine, hess_fine,
    )

    for send in sends:
        send.wait_recv()

    @pl.when(jnp.logical_or(c == 1, has_up))
    def _():
        @pl.when(jnp.logical_or(c == 0, has_down))
        def _():
            for j in range(chunks):
                for index in range(2):
                    pltpu.make_async_remote_copy(
                        src_ref=ups[j].src_ref, dst_ref=ups[j].dst_ref,
                        send_sem=csend.at[4 * j + 2], recv_sem=crecv.at[4 * j + 2 + index],
                        device_id={"row": r, "col": other}, device_id_type=MESH,
                    ).wait_recv()

    for begin in range(0, tiles, CHUNK):
        end = begin + CHUNK + (1 if begin + CHUNK == tiles else 0)
        vertical_pass(cext, a_coarse, jnp.ones((1, LANE), F32), begin, end)
    horizontal_pass(0, strip + 8, 0, tiles)
    responses(
        strip, tiles, 80.0, 200000.0,
        row_mask(strip, jnp.logical_or(has_up, c == 1), jnp.logical_or(has_down, c == 0)),
        None, dog_coarse, hess_coarse,
    )

    @pl.when(has_down)
    def _():
        to_down_corner.wait_send()
        for send in to_down + downs:
            send.wait_send()

    @pl.when(has_up)
    def _():
        to_up_corner.wait_send()
        for send in to_up + ups:
            send.wait_send()

    for send in sends:
        send.wait_send()


def solution(mesh):
    rows_total = mesh.shape["row"]

    def local(image):
        tile_rows, tile_cols = image.shape
        strip = tile_rows // 4
        tiles = tile_cols // LANE
        fine_in = ring_inputs(tile_rows + 2 * RIM, RIM)
        coarse_in = ring_inputs(3 * strip, strip)
        a_fine = row_weights(
            np.concatenate(
                [vertical_matrix(2.0 * np.arange(tile_rows // 2), fine_in, SIGMAS[4])]
                + [vertical_matrix(ring_rows(tile_rows), fine_in, s) for s in SIGMAS]
            )
        )
        a_coarse = row_weights(
            np.concatenate([vertical_matrix(ring_rows(strip), coarse_in, s) for s in SIGMAS])
        )
        window = np.arange(2 * LANE, dtype=np.float64)[:, None] - HALF
        g_level = np.stack(
            [column_weights(taps_at(s, window - np.arange(LANE)[None, :])) for s in SIGMAS]
        )
        wider = np.arange(3 * LANE, dtype=np.float64)[:, None] - HALF
        g_base = column_weights(taps_at(SIGMAS[4], wider - 2.0 * np.arange(LANE)[None, :]))

        vmem = pl.BlockSpec(memory_space=pltpu.VMEM)
        ring = tile_rows + 8
        wide = tile_cols + LANE
        chunks = tiles // CHUNK
        return pl.pallas_call(
            functools.partial(kernel, rows_total),
            out_shape=(
                jax.ShapeDtypeStruct((4, tile_rows, tile_cols), BF),
                jax.ShapeDtypeStruct((2, tile_rows, tile_cols), BF),
                jax.ShapeDtypeStruct((4, strip, tile_cols), BF),
                jax.ShapeDtypeStruct((2, strip, tile_cols), BF),
            ),
            in_specs=[pl.BlockSpec(memory_space=pltpu.HBM)] * 5,
            out_specs=(vmem,) * 4,
            scratch_shapes=[
                pltpu.VMEM((tile_rows + 2 * RIM, wide), F32),
                pltpu.VMEM((3 * strip, wide), F32),
                pltpu.VMEM((a_fine.shape[0], wide), F32),
                pltpu.VMEM((LEVELS, (tiles + 1) * ring, LANE), F32),
                pltpu.VMEM((2, (tiles + 1) * ring, LANE), F32),
                pltpu.VMEM((tile_rows // 2, tile_cols // 2), F32),
                pltpu.VMEM(a_fine.shape, BF),
                pltpu.VMEM(a_coarse.shape, BF),
                pltpu.VMEM(g_level.shape, BF),
                pltpu.VMEM(g_base.shape, BF),
                pltpu.SemaphoreType.DMA((5,)),
                pltpu.SemaphoreType.DMA((2 * chunks + 3,)),
                pltpu.SemaphoreType.DMA((2 * chunks + 3,)),
                pltpu.SemaphoreType.DMA((4 * chunks,)),
                pltpu.SemaphoreType.DMA((4 * chunks,)),
            ],
            compiler_params=pltpu.CompilerParams(
                collective_id=0, has_side_effects=True, vmem_limit_bytes=62500000
            ),
        )(image, a_fine, a_coarse, g_level, g_base)

    return jax.shard_map(
        local,
        mesh=mesh,
        in_specs=(P(("slab", "row"), "col"),),
        out_specs=(
            P(None, ("slab", "row"), "col"),
            P(None, ("slab", "row"), "col"),
            P(None, ("slab", "row", "col"), None),
            P(None, ("slab", "row", "col"), None),
        ),
        check_vma=False,
    )
```
